32 devices in a mesh: seq: 8 (over y, x, core), head: 4 (over z).
Axes of the slice: x: 2, y: 2, z: 4, core: 2. Of those that a mesh axis runs over, the one named last changes fastest.
Arguments:
- query_rows: bfloat16 [2048, 1024], P('seq', 'head'), may hold values from -6 to 6
- key_rows: bfloat16 [2048, 1024], P('seq', 'head'), may hold values from -6 to 6
- value_rows: bfloat16 [2048, 2048], P('seq', 'head'), may hold values from -6 to 6
- output_gate: bfloat16 [2048, 2048], P('seq', 'head'), may hold values from -6 to 6
- write_rate: float32 [16, 2048], P('head', 'seq'), may hold values from 0.05 to 1
- log_decay: float32 [16, 2048], P('head', 'seq'), may hold values from -1.2 to 0, as said below
- out_weight: bfloat16 [2048, 2048], P(None, 'head'), may hold values from -0.125 to 0.125
- out_cotangent: bfloat16 [2048, 2048], P('seq', 'head'), may hold values from -6 to 6
- block_response: int32 [24], replicated, may hold values from 0 to 15, as said below
- prefix_owner: int32 [8], replicated, may hold values from 0 to 7, each once
Outputs:
- layer_out: bfloat16 [2048, 2048], P('seq', 'head')
- grad_query: float32 [2048, 1024], P('seq', 'head')
- grad_key: float32 [2048, 1024], P('seq', 'head')
- grad_value: float32 [2048, 2048], P('seq', 'head')
- grad_gate: float32 [2048, 2048], P('seq', 'head')
- grad_write: float32 [16, 2048], P('head', 'seq')
- grad_decay: float32 [16, 2048], P('head', 'seq')
- grad_weight: float32 [2048, 2048], P('seq', 'head')
The draws below stay inside these ranges and needn't reach their ends.
Inputs may be any that keep to these rules, and one draw needn't show every extreme that they name: `block_response`: blocks of one response are consecutive and lie within the 3 blocks of one index of seq; responses appear in increasing order; each response has 1 to 3 blocks and one has exactly 3; every response of 0 to 15 appears. `prefix_owner`: each index of seq holds exactly one prompt's prefix. `log_decay`: every entry is negative.
All inputs are finite; a program needn't handle non-finite values.
Results may differ from the reference program's by a relative error of at most 0.015.
Values may be sent and summed in bfloat16 or wider, within the bound.
No kernel may reach another device: no remote copies, remote signals or barrier semaphores. Data moves between devices by JAX's collectives and lax.ppermute only.
A program may use at most 64 MiB of HBM per device.

```python
import math
from functools import partial
import jax
import jax.numpy as jnp
from jax import lax

D = 2048
VALUE_HEADS = 16
K_HEADS = 8
DK = 128
DV = 128
SPAN = 64
PREFIX = 64
BLK_DEV = 3
RESP_PER = 2
MOST = 3
ROWS = 256
TOKEN_ROWS = 2048
PROMPTS = 8
RESPONSES = 16
NBLK = 24
KEYS = 1024
VALUE = 2048
N_SEQ = 8


def draw_log_decay(key, part):
    chain_length = PREFIX + MOST * SPAN
    every_key = jax.random.split(key, 6)
    head_shape = (VALUE_HEADS, 1)
    base_rate = jnp.exp(jax.random.uniform(every_key[0], head_shape, jnp.float32, math.log(0.1 / chain_length), math.log(1.0 / 30.0)))
    block_total = TOKEN_ROWS // SPAN
    block_factor = jnp.exp(jax.random.uniform(every_key[3], (VALUE_HEADS, block_total, 1), jnp.float32, -0.7, 0.7))
    token_factor = jnp.exp(jax.random.uniform(every_key[4], (VALUE_HEADS, block_total, SPAN), jnp.float32, -0.7, 0.7))
    spike_key, depth_random_key = jax.random.split(every_key[5])
    spike_groups = jax.random.uniform(spike_key, (VALUE_HEADS, TOKEN_ROWS), jnp.float32) < 3.0 / chain_length
    spike_depth = jax.random.uniform(depth_random_key, (VALUE_HEADS, TOKEN_ROWS), jnp.float32, 0.2, 0.7)
    decay_speed = (base_rate[:, :, None] * block_factor * token_factor).reshape(VALUE_HEADS, TOKEN_ROWS)
    decay_speed = decay_speed + jnp.where(spike_groups, spike_depth, 0.0)
    return -decay_speed


def draw_block_response(key, part):
    lone_key, order_key = jax.random.split(jax.random.fold_in(key, 17))
    spare = BLK_DEV - 1
    cand_total = N_SEQ * spare
    extra = RESPONSES - N_SEQ
    lone = jax.random.randint(lone_key, (), 0, N_SEQ).astype(jnp.int32)
    order = jax.random.permutation(order_key, cand_total).astype(jnp.int32)
    cand_ids = jnp.arange(cand_total, dtype=jnp.int32)
    cand_dev = cand_ids // spare
    score = order + jnp.where(cand_dev == lone, cand_total, 0).astype(jnp.int32)
    ranks = jnp.argsort(jnp.argsort(score))
    chosen = (ranks < extra).astype(jnp.int32)
    flat_pos = cand_dev * BLK_DEV + cand_ids % spare + 1
    starts = jnp.zeros((NBLK,), jnp.int32).at[flat_pos].set(chosen)
    first_pos = jnp.arange(N_SEQ, dtype=jnp.int32) * BLK_DEV
    starts = starts.at[first_pos].set(1)
    return (jnp.cumsum(starts) - 1).astype(jnp.int32)


def shard_levels(rng, extent, cuts, low, high):
    def one(position, blocks):
        steps = jax.random.uniform(jax.random.fold_in(jax.random.fold_in(rng, 6), position), (blocks,), jnp.float32, low / len(cuts), high / len(cuts))
        return jnp.repeat(jnp.exp(steps), extent[position] // blocks).reshape((-1,) + (1,) * (len(extent) - position - 1))

    gain = one(*cuts[0])
    for cut in cuts[1:]:
        gain = gain * one(*cut)
    return gain


def gaussian(own_key, dims, scale, reach, cuts=(), kind=jnp.bfloat16):
    values = jax.random.normal(own_key, dims, jnp.float32) * scale
    if len(cuts) > 0:
        values = shard_levels(own_key, dims, cuts, -0.22, 0.18) * values
    return jnp.clip(values, min=-reach, max=reach).astype(kind)


def setup_inputs(seed: int = 0) -> dict:
    streams_of = jax.random.split(jax.random.key(seed), 11)
    return {
        "query_rows": gaussian(streams_of[0], (TOKEN_ROWS, KEYS), 1.0, 6.0, ((0, 8), (1, 4))),
        "key_rows": gaussian(streams_of[1], (TOKEN_ROWS, KEYS), 1.0, 6.0, ((0, 8), (1, 4))),
        "value_rows": gaussian(streams_of[2], (TOKEN_ROWS, VALUE), 1.0, 6.0, ((0, 8), (1, 4))),
        "output_gate": gaussian(streams_of[3], (TOKEN_ROWS, VALUE), 1.0, 6.0, ((0, 8), (1, 4))),
        "write_rate": jnp.clip(0.05 + 0.95 * jax.random.uniform(streams_of[4], (VALUE_HEADS, TOKEN_ROWS), jnp.float32) ** shard_levels(streams_of[4], (VALUE_HEADS, TOKEN_ROWS), ((0, 4), (1, 8)), -0.2, 0.2), 0.05, 1.0),
        "log_decay": draw_log_decay(jax.random.fold_in(streams_of[10], 71), 0),
        "out_weight": gaussian(streams_of[6], (D, VALUE), VALUE ** -0.5, 0.125, ((1, 4),)),
        "out_cotangent": gaussian(streams_of[7], (TOKEN_ROWS, D), 1.0, 6.0, ((0, 8), (1, 4))),
        "block_response": draw_block_response(jax.random.fold_in(streams_of[10], 71), 0),
        "prefix_owner": jax.random.permutation(streams_of[9], PROMPTS).astype(jnp.int32),
    }


highest = lax.Precision.HIGHEST
tiny_eps = 1e-06

def unit_rows(raw_rows):
    return raw_rows * lax.rsqrt(lax.optimization_barrier(jnp.sum(raw_rows * raw_rows, axis=-1, keepdims=True)) + tiny_eps)

def span_parts(query_unit, key_unit, value_part, write_part, decay_part):
    span_len = decay_part.shape[-1]
    dim_key = key_unit.shape[-1]
    cumulative = jnp.cumsum(decay_part, axis=-1)
    row_ids = lax.broadcasted_iota(jnp.int32, (span_len, span_len), 0)
    col_ids = lax.broadcasted_iota(jnp.int32, (span_len, span_len), 1)
    strict = row_ids > col_ids
    causal = row_ids >= col_ids
    spread = cumulative[..., :, None] - cumulative[..., None, :]
    below_diag = jnp.where(strict, jnp.exp(jnp.where(strict, spread, 0.0)), 0.0)
    within = jnp.where(causal, jnp.exp(jnp.where(causal, spread, 0.0)), 0.0)
    key_key = jnp.einsum('...ik,...jk->...ij', key_unit, key_unit, precision=highest)
    system = jnp.eye(span_len, dtype=jnp.float32) + write_part[..., :, None] * below_diag * key_key
    growth = jnp.exp(cumulative)
    right_side = jnp.concatenate([(write_part * growth)[..., None] * key_unit, write_part[..., None] * value_part], axis=-1)
    solved = lax.linalg.triangular_solve(system, right_side, left_side=True, lower=True, unit_diagonal=True)
    weights_w = solved[..., :dim_key]
    base_u = solved[..., dim_key:]
    query_key = jnp.einsum('...ik,...jk->...ij', query_unit, key_unit, precision=highest) * within
    remain = jnp.exp(cumulative[..., -1:] - cumulative)
    key_tail = remain[..., None] * key_unit
    transfer = growth[..., -1][..., None, None] * jnp.eye(dim_key, dtype=jnp.float32) - jnp.einsum('...ck,...cl->...kl', weights_w, key_tail, precision=highest)
    offset = jnp.einsum('...cv,...ck->...vk', base_u, key_tail, precision=highest)
    return (transfer, offset, weights_w, base_u, query_key, growth, query_unit)

def span_apply(span_terms, state_in):
    transfer, offset, weights_w, base_u, query_key, growth, query_unit = span_terms
    update = base_u - jnp.einsum('...ck,...vk->...cv', weights_w, state_in, precision=highest)
    block_out = growth[..., None] * jnp.einsum('...ck,...vk->...cv', query_unit, state_in, precision=highest)
    block_out = block_out + jnp.einsum('...ij,...jv->...iv', query_key, update, precision=highest)
    state_out = jnp.einsum('...vk,...kl->...vl', state_in, transfer, precision=highest) + offset
    return (block_out, state_out)

def prefix_region(head_array):
    feat_width = head_array.shape[3]
    piece = jnp.transpose(head_array[:, :, :PREFIX], (1, 0, 2, 3)).reshape(N_SEQ * VALUE_HEADS, PREFIX, feat_width)
    return jnp.transpose(piece.reshape(N_SEQ * VALUE_HEADS, PREFIX // SPAN, SPAN, feat_width), (1, 0, 2, 3))

def answer_region(head_array):
    feat_width = head_array.shape[3]
    piece = head_array[:, :, PREFIX:].reshape(VALUE_HEADS, N_SEQ, BLK_DEV, SPAN, feat_width)
    return jnp.transpose(piece, (1, 2, 0, 3, 4)).reshape(N_SEQ * BLK_DEV, VALUE_HEADS, SPAN, feat_width)

def slot_major(flat_blocks):
    grouped_blocks = flat_blocks.reshape((N_SEQ, BLK_DEV) + flat_blocks.shape[1:])
    return jnp.swapaxes(grouped_blocks, 0, 1)

def gated_layer(query32, key32, value32, gate32, write_rate, log_decay, block_response, prefix_owner):
    query_unit = unit_rows(query32.reshape(TOKEN_ROWS, K_HEADS, DK)) * DK ** (-0.5)
    key_unit = unit_rows(key32.reshape(TOKEN_ROWS, K_HEADS, DK))
    query_unit = jnp.repeat(jnp.transpose(query_unit, (1, 0, 2)), VALUE_HEADS // K_HEADS, axis=0)
    key_unit = jnp.repeat(jnp.transpose(key_unit, (1, 0, 2)), VALUE_HEADS // K_HEADS, axis=0)
    values = jnp.transpose(value32.reshape(TOKEN_ROWS, VALUE_HEADS, DV), (1, 0, 2))
    grouped = (query_unit.reshape(VALUE_HEADS, N_SEQ, ROWS, DK), key_unit.reshape(VALUE_HEADS, N_SEQ, ROWS, DK), values.reshape(VALUE_HEADS, N_SEQ, ROWS, DV), write_rate.reshape(VALUE_HEADS, N_SEQ, ROWS, 1), log_decay.reshape(VALUE_HEADS, N_SEQ, ROWS, 1))
    prefix_in = tuple((prefix_region(item) for item in grouped))
    prefix_in = prefix_in[:3] + (prefix_in[3][..., 0], prefix_in[4][..., 0])

    def advance(state_in, block_in):
        block_out, state_out = span_apply(span_parts(*block_in), state_in)
        return (state_out, block_out)
    last_state, prefix_outs = lax.scan(advance, jnp.zeros((N_SEQ * VALUE_HEADS, DV, DK), jnp.float32), prefix_in)
    last_state = last_state.reshape(N_SEQ, VALUE_HEADS, DV, DK)
    rounded = lax.optimization_barrier(last_state.astype(jnp.bfloat16)).astype(jnp.float32)
    states_all = last_state + lax.stop_gradient(rounded - last_state)
    answer_in = tuple((answer_region(item) for item in grouped))
    answer_in = answer_in[:3] + (answer_in[3][..., 0], answer_in[4][..., 0])
    answer_in = tuple((slot_major(item) for item in answer_in))
    block_flags = jnp.concatenate([jnp.ones((1,), dtype=bool), block_response[1:] != block_response[:-1]])
    owners = jnp.take(prefix_owner, block_response // RESP_PER).astype(jnp.int32)
    slot_flags = slot_major(block_flags)
    slot_owners = slot_major(owners)

    def respond(state_in, block_in):
        inputs_here, block_flag, block_owner = block_in
        chosen = jnp.take(states_all, block_owner, axis=0)
        state_in = jnp.where(block_flag[:, None, None, None], chosen, state_in)
        block_out, state_out = span_apply(span_parts(*inputs_here), state_in)
        return (state_out, block_out)
    ignored, answer_outs = lax.scan(respond, jnp.zeros((N_SEQ, VALUE_HEADS, DV, DK), jnp.float32), (answer_in, slot_flags, slot_owners))
    answer_outs = jnp.swapaxes(answer_outs, 0, 1).reshape(N_SEQ * BLK_DEV, VALUE_HEADS, SPAN, DV)
    prefix_rows = jnp.transpose(prefix_outs.reshape(PREFIX // SPAN, N_SEQ, VALUE_HEADS, SPAN, DV), (1, 0, 3, 2, 4)).reshape(N_SEQ, PREFIX, VALUE)
    answer_rows = jnp.transpose(answer_outs.reshape(N_SEQ, BLK_DEV, VALUE_HEADS, SPAN, DV), (0, 1, 3, 2, 4)).reshape(N_SEQ, BLK_DEV * SPAN, VALUE)
    outs_all = jnp.concatenate([prefix_rows, answer_rows], axis=1).reshape(TOKEN_ROWS, VALUE_HEADS, DV)
    inv_scale = lax.rsqrt(lax.optimization_barrier(jnp.mean(outs_all * outs_all, axis=-1, keepdims=True)) + tiny_eps)
    gated_rows = outs_all * inv_scale * jax.nn.silu(gate32.reshape(TOKEN_ROWS, VALUE_HEADS, DV))
    return gated_rows.reshape(TOKEN_ROWS, VALUE)

def reference(query_rows, key_rows, value_rows, output_gate, write_rate, log_decay, out_weight, out_cotangent, block_response, prefix_owner):
    layer_fn = partial(gated_layer, block_response=block_response, prefix_owner=prefix_owner)
    floats = (query_rows.astype(jnp.float32), key_rows.astype(jnp.float32), value_rows.astype(jnp.float32), output_gate.astype(jnp.float32), write_rate, log_decay)
    normed, pullback = jax.vjp(layer_fn, *floats)
    rounded = normed.astype(jnp.bfloat16)
    layer_out = jnp.dot(rounded.astype(jnp.float32), out_weight.T.astype(jnp.float32), preferred_element_type=jnp.float32).astype(jnp.bfloat16)
    grad_normed = jnp.dot(out_cotangent.astype(jnp.float32), out_weight.astype(jnp.float32), preferred_element_type=jnp.float32)
    grad_weight = jnp.dot(out_cotangent.T.astype(jnp.float32), rounded.astype(jnp.float32), preferred_element_type=jnp.float32)
    all_grads = pullback(grad_normed)
    return (layer_out, all_grads[0], all_grads[1], all_grads[2], all_grads[3], all_grads[4], all_grads[5], grad_weight)
```

```python
from functools import partial

import jax
import jax.numpy as jnp
from jax import lax
from jax.experimental import pallas as pl
from jax.experimental.pallas import tpu as pltpu
from jax.sharding import PartitionSpec as P

DK = 128
DV = 128
SPAN = 64
RESP_PER = 2
EPS = 1e-06
F32 = jnp.float32
BF16 = jnp.bfloat16
ROW_G, ROW_B, ROW_RK, ROW_RQ, ROW_END = 0, 8, 16, 24, 32


def dot_nn(a, b):
    return lax.dot_general(a, b, (((1,), (0,)), ((), ())), preferred_element_type=F32)


def dot_nt(a, b):
    return lax.dot_general(a, b, (((1,), (1,)), ((), ())), preferred_element_type=F32)


def dot_tn(a, b):
    return lax.dot_general(a, b, (((0,), (0,)), ((), ())), preferred_element_type=F32)


def halves(x):
    high = x.astype(BF16)
    return high, (x - high.astype(F32)).astype(BF16)


def dot3(a, b):
    ah, al = halves(a)
    bh, bl = halves(b)
    return dot_nn(ah, bh) + (dot_nn(ah, bl) + dot_nn(al, bh))


def iota2(shape, dim):
    return lax.broadcasted_iota(jnp.int32, shape, dim)


def unit_lower_inverse(lower, upto):
    size = lower.shape[0]
    ri, ci = iota2(lower.shape, 0), iota2(lower.shape, 1)
    eye = (ri == ci).astype(F32)
    inv = eye - jnp.where((ri // 2) == (ci // 2), lower, 0.0)
    step = 2
    while step < upto:
        joins = ((ri // (2 * step)) == (ci // (2 * step))) & ((ri // step) != (ci // step))
        off = jnp.where(joins, lower, 0.0).astype(BF16)
        inv16 = inv.astype(BF16)
        inv = inv - dot_nn(inv16, dot_nn(off, inv16).astype(BF16))
        step *= 2
    residual = (eye - inv) - dot3(lower, inv)
    return inv + dot_nn(inv.astype(BF16), residual.astype(BF16))


def response_ids(br_ref, blocks):
    base = lax.axis_index("seq") * blocks
    return [br_ref[base + b] for b in range(blocks)]


def segment_of(pos, ids):
    seg = jnp.full(pos.shape, -1, jnp.int32)
    for b, name in enumerate(ids):
        seg = jnp.where(pos // SPAN == b + 1, name, seg)
    return seg


def segment_masks(rows, ids):
    ri, ci = iota2((rows, rows), 0), iota2((rows, rows), 1)
    same = segment_of(ri, ids) == segment_of(ci, ids)
    return same, ri, ci


def exact_pieces(x):
    one = x.astype(BF16).astype(F32)
    two = (x - one).astype(BF16).astype(F32)
    three = x - one - two
    return jnp.concatenate([one, two, three, jnp.zeros_like(x)], axis=0).astype(BF16)


def exact_rows_dot(x, mask):
    parts = dot_nn(exact_pieces(x), mask)
    return parts[0:8] + (parts[8:16] + parts[16:24])


def col(cols, lane):
    return cols[:, lane : lane + 1]


def prefix_kernel(br_ref, q_ref, k_ref, v_ref, w_ref, d_ref, rows_ref, cols_ref, state_ref):
    rows = q_ref.shape[0]
    heads = w_ref.shape[0]
    key_heads = q_ref.shape[1] // DK
    rep = heads // key_heads
    blocks = rows // SPAN - 1
    ids = response_ids(br_ref, blocks)
    same, ri, ci = segment_masks(rows, ids)
    upto = (same & (ri <= ci)).astype(F32).astype(BF16)
    pad = jnp.zeros((8 - heads, rows), F32)
    g8 = exact_rows_dot(jnp.concatenate([d_ref[...], pad], axis=0), upto)
    b8 = jnp.concatenate([w_ref[...], pad], axis=0)
    lane = iota2((rows, 128), 1)
    norms = jnp.zeros((rows, 128), F32)
    for kh in range(key_heads):
        kf = k_ref[:, kh * DK : (kh + 1) * DK].astype(F32)
        qf = q_ref[:, kh * DK : (kh + 1) * DK].astype(F32)
        rk = lax.rsqrt(jnp.sum(kf * kf, axis=1, keepdims=True) + EPS)
        rq = lax.rsqrt(jnp.sum(qf * qf, axis=1, keepdims=True) + EPS) * (DK**-0.5)
        norms = jnp.where(lane == ROW_RK + kh, rk, norms)
        norms = jnp.where(lane == ROW_RQ + kh, rq, norms)
    norms_t = norms.T
    rows_ref[...] = jnp.concatenate([g8, b8, norms_t[ROW_RK:ROW_END]], axis=0)
    first = jnp.concatenate([g8, b8, jnp.zeros((112, rows), F32)], axis=0)
    cols = first.T + norms
    cols_ref[...] = cols

    n = rep * SPAN
    pi, pj = iota2((n, n), 0), iota2((n, n), 1)
    strict = (pi > pj) & (pi // SPAN == pj // SPAN)
    for kh in range(key_heads):
        kp = k_ref[0:SPAN, kh * DK : (kh + 1) * DK]
        k2 = jnp.concatenate([kp] * rep, axis=0)

        def stack(base, each):
            return jnp.concatenate(
                [cols[0:SPAN, base + (kh * rep + r if each else kh) :][:, 0:1] for r in range(rep)],
                axis=0,
            )

        g2 = stack(ROW_G, True)
        b2 = stack(ROW_B, True)
        rk2 = stack(ROW_RK, False)
        last = jnp.concatenate(
            [jnp.broadcast_to(g2[(r + 1) * SPAN - 1 : (r + 1) * SPAN], (SPAN, 1)) for r in range(rep)],
            axis=0,
        )
        gm = jnp.broadcast_to(g2, (n, n))
        rm = jnp.broadcast_to(rk2, (n, n))
        decay = jnp.exp(jnp.where(strict, gm - gm.T, -1e30))
        lower = dot_nt(k2, k2) * (rm * rm.T) * (b2 * decay)
        inv = unit_lower_inverse(lower, SPAN)
        v2 = jnp.concatenate(
            [v_ref[:, (kh * rep + r) * DV : (kh * rep + r + 1) * DV] for r in range(rep)], axis=0
        ).astype(F32)
        u2 = dot3(inv, b2 * v2)
        weighted = u2 * (jnp.exp(last - g2) * rk2)
        wh, wl = halves(weighted)
        for r in range(rep):
            cut = slice(r * SPAN, (r + 1) * SPAN)
            state_ref[kh * rep + r] = (dot_tn(kp, wh[cut]) + dot_tn(kp, wl[cut])).astype(BF16)


def system_kernel(br_ref, q_ref, k_ref, rows_ref, cols_ref, n_ref, nt_ref, m_ref, mt_ref):
    rows = q_ref.shape[0]
    rep = n_ref.shape[0]
    kh = pl.program_id(0)
    ids = response_ids(br_ref, rows // SPAN - 1)
    same, ri, ci = segment_masks(rows, ids)
    causal = same & (ri >= ci)
    causal_t = same & (ri <= ci)
    strict = same & (ri > ci)
    q, k = q_ref[...], k_ref[...]
    lane = iota2((rows, 128), 1)
    cols = cols_ref[...]

    def pick(base):
        return jnp.sum(jnp.where(lane == base, cols, 0.0), axis=1, keepdims=True)

    def pick_row(base):
        return rows_ref[pl.ds(base, 1), :]

    rk_c, rq_c = pick(ROW_RK + kh), pick(ROW_RQ + kh)
    rk_r, rq_r = pick_row(ROW_RK + kh), pick_row(ROW_RQ + kh)
    kk = dot_nt(k, k) * (rk_c * rk_r)
    qk = dot_nt(q, k) * (rq_c * rk_r)
    kq = dot_nt(k, q) * (rk_c * rq_r)
    half = rows // 2
    for r in range(rep):
        h = kh * rep + r
        g_c, b_c = pick(ROW_G + h), pick(ROW_B + h)
        g_r = pick_row(ROW_G + h)
        diff = g_c - g_r
        decay = jnp.exp(jnp.where(causal, diff, -1e30))
        decay_t = jnp.exp(jnp.where(causal_t, -diff, -1e30))
        m_ref[r] = (qk * decay).astype(BF16)
        mt_ref[r] = (kq * decay_t).astype(BF16)
        lower = jnp.where(strict, kk * (b_c * decay), 0.0)
        t11 = unit_lower_inverse(lower[:half, :half], half)
        t22 = unit_lower_inverse(lower[half:, half:], half)
        t21 = -dot3(t22, dot3(lower[half:, :half], t11))
        eye = (iota2((half, half), 0) == iota2((half, half), 1)).astype(F32)
        zero = jnp.zeros((half, half), F32)
        n_ref[r, :half, :half] = (t11 - eye).astype(BF16)
        n_ref[r, :half, half:] = zero.astype(BF16)
        n_ref[r, half:, :half] = t21.astype(BF16)
        n_ref[r, half:, half:] = (t22 - eye).astype(BF16)
        nt_ref[r, :half, :half] = (t11 - eye).T.astype(BF16)
        nt_ref[r, half:, :half] = zero.astype(BF16)
        nt_ref[r, :half, half:] = t21.T.astype(BF16)
        nt_ref[r, half:, half:] = (t22 - eye).T.astype(BF16)


def forward_kernel(
    br_ref, po_ref, q_ref, k_ref, v_ref, z_ref, cols_ref, n_ref, m_ref, st_ref,
    normed_ref, o_ref, u_ref, r_ref, y_ref,
):
    rows = q_ref.shape[0]
    h = pl.program_id(0)
    blocks = rows // SPAN - 1
    ids = response_ids(br_ref, blocks)
    lane = iota2((rows, 128), 1)
    cols = cols_ref[...]

    def pick(base):
        return jnp.sum(jnp.where(lane == base, cols, 0.0), axis=1, keepdims=True)

    kh = h // HEAD_REP[0]
    g_c, b_c = pick(ROW_G + h), pick(ROW_B + h)
    rk_c, rq_c = pick(ROW_RK + kh), pick(ROW_RQ + kh)
    growth = jnp.exp(g_c)
    zs, ys = [jnp.zeros((SPAN, DV), F32)], [jnp.zeros((SPAN, DV), F32)]
    for b in range(blocks):
        state = st_ref[po_ref[ids[b] // RESP_PER], 0]
        cut = slice((b + 1) * SPAN, (b + 2) * SPAN)
        zs.append(dot_nn(k_ref[cut, :], state))
        ys.append(dot_nn(q_ref[cut, :], state))
    start_v = jnp.concatenate(zs, axis=0) * (growth * rk_c)
    start_o = jnp.concatenate(ys, axis=0) * (growth * rq_c)
    right = b_c * (v_ref[...].astype(F32) - start_v)
    update = right + dot_nn(n_ref[0], right.astype(BF16))
    update16 = update.astype(BF16)
    out = start_o + dot_nn(m_ref[0], update16)
    inv = lax.rsqrt(jnp.mean(out * out, axis=1, keepdims=True) + EPS)
    gate = z_ref[...].astype(F32)
    normed_ref[...] = (out * inv * (gate / (1.0 + jnp.exp(-gate)))).astype(BF16)
    o_ref[...] = out
    u_ref[0] = update16
    r_ref[0] = right
    y_ref[0] = start_o


def backward_state_kernel(
    br_ref, po_ref, q_ref, k_ref, z_ref, gn_ref, o_ref, cols_ref, nt_ref, mt_ref,
    dz_ref, do_ref, dr_ref, gs_ref,
):
    rows = q_ref.shape[0]
    h = pl.program_id(0)
    kh = h // HEAD_REP[0]
    blocks = rows // SPAN - 1
    ids = response_ids(br_ref, blocks)
    lane = iota2((rows, 128), 1)
    cols = cols_ref[...]

    def pick(base):
        return jnp.sum(jnp.where(lane == base, cols, 0.0), axis=1, keepdims=True)

    g_c, b_c = pick(ROW_G + h), pick(ROW_B + h)
    rk_c, rq_c = pick(ROW_RK + kh), pick(ROW_RQ + kh)
    growth = jnp.exp(g_c)
    out = o_ref[...]
    gate = z_ref[...].astype(F32)
    gn = gn_ref[...]
    inv = lax.rsqrt(jnp.mean(out * out, axis=1, keepdims=True) + EPS)
    sig = 1.0 / (1.0 + jnp.exp(-gate))
    silu = gate * sig
    unit = out * inv
    dz_ref[...] = gn * unit * (sig * (1.0 + gate * (1.0 - sig)))
    dh = gn * silu
    dout = inv * (dh - unit * jnp.mean(dh * unit, axis=1, keepdims=True))
    do_ref[0] = dout
    dupdate = dot_nn(mt_ref[0], dout.astype(BF16))
    dright = dupdate + dot_nn(nt_ref[0], dupdate.astype(BF16))
    dr_ref[0] = dright
    dkey = (dright * (-(b_c * growth * rk_c))).astype(BF16)
    dqry = (dout * (growth * rq_c)).astype(BF16)
    gs_ref[...] = jnp.zeros(gs_ref.shape, BF16)
    parts = []
    owners = [po_ref[ids[b] // RESP_PER] for b in range(blocks)]
    for b in range(blocks):
        cut = slice((b + 1) * SPAN, (b + 2) * SPAN)
        parts.append(dot_tn(k_ref[cut, :], dkey[cut]) + dot_tn(q_ref[cut, :], dqry[cut]))
    for b in range(blocks):
        total = parts[b]
        for c in range(blocks):
            if c != b:
                total = total + jnp.where(owners[c] == owners[b], 1.0, 0.0) * parts[c]
        gs_ref[owners[b], 0] = total.astype(BF16)


def backward_rest_kernel(
    br_ref, po_ref, q_ref, k_ref, v_ref, rows_ref, cols_ref, st_ref, do_ref, dr_ref, u_ref,
    r_ref, y_ref, dq_ref, dk_ref, dv_ref, dw_ref, dd_ref, acc_ref,
):
    rows = q_ref.shape[0]
    rep = u_ref.shape[0]
    heads = dw_ref.shape[0]
    kh = pl.program_id(0)
    blocks = rows // SPAN - 1
    ids = response_ids(br_ref, blocks)
    same, ri, ci = segment_masks(rows, ids)
    causal = same & (ri >= ci)
    causal_t = same & (ri <= ci)
    off_diag = ri != ci
    lane = iota2((rows, 128), 1)
    cols = cols_ref[...]

    def pick(base):
        return jnp.sum(jnp.where(lane == base, cols, 0.0), axis=1, keepdims=True)

    def pick_row(base):
        return rows_ref[pl.ds(base, 1), :]

    @pl.when(kh == 0)
    def _():
        acc_ref[...] = jnp.zeros_like(acc_ref)

    q, k = q_ref[...], k_ref[...]
    rk_c, rq_c = pick(ROW_RK + kh), pick(ROW_RQ + kh)
    rk_r, rq_r = pick_row(ROW_RK + kh), pick_row(ROW_RQ + kh)
    kk = dot_nt(k, k)
    qk = dot_nt(q, k)
    kq = dot_nt(k, q)
    dqh = jnp.zeros((rows, DK), F32)
    dkh = jnp.zeros((rows, DK), F32)
    for r in range(rep):
        h = kh * rep + r
        g_c, b_c = pick(ROW_G + h), pick(ROW_B + h)
        g_r, b_r = pick_row(ROW_G + h), pick_row(ROW_B + h)
        growth = jnp.exp(g_c)
        diff = g_c - g_r
        decay = jnp.exp(jnp.where(causal, diff, -1e30))
        decay_t = jnp.exp(jnp.where(causal_t, -diff, -1e30))
        dout, dright, right, start_o = do_ref[r], dr_ref[r], r_ref[r], y_ref[r]
        u16 = u_ref[r]
        do16, dr16 = dout.astype(BF16), dright.astype(BF16)
        p1 = dot_nt(do16, u16) * (decay * rk_r)
        p1t = dot_nt(u16, do16) * (decay_t * rq_r)
        strict_w = jnp.where(off_diag, decay, 0.0)
        strict_wt = jnp.where(off_diag, decay_t, 0.0)
        p2 = dot_nt(dr16, u16) * (strict_w * (-b_c) * rk_r)
        p2t = dot_nt(u16, dr16) * (strict_wt * (-b_r) * rk_r)
        e2sum = jnp.sum(p2 * kk, axis=1, keepdims=True) * rk_c
        e1sum = jnp.sum(p1 * qk, axis=1, keepdims=True) * rq_c
        tsum = jnp.sum(p1t * kq + p2t * kk, axis=1, keepdims=True) * rk_c
        dqh = dqh + dot_nn(p1.astype(BF16), k)
        dkh = dkh + dot_nn((p2 + p2t).astype(BF16), k) + dot_nn(p1t.astype(BF16), q)
        dkey = (dright * (-(b_c * growth))).astype(BF16)
        dqry = (dout * growth).astype(BF16)
        dks, dqs = [jnp.zeros((SPAN, DK), F32)], [jnp.zeros((SPAN, DK), F32)]
        for b in range(blocks):
            state = st_ref[po_ref[ids[b] // RESP_PER], r]
            cut = slice((b + 1) * SPAN, (b + 2) * SPAN)
            dks.append(dot_nt(dkey[cut], state))
            dqs.append(dot_nt(dqry[cut], state))
        dkh = dkh + jnp.concatenate(dks, axis=0)
        dqh = dqh + jnp.concatenate(dqs, axis=0)
        vf = v_ref[:, r * DV : (r + 1) * DV].astype(F32)
        dr_r = jnp.sum(dright * right, axis=1, keepdims=True)
        dr_v = jnp.sum(dright * vf, axis=1, keepdims=True)
        do_y = jnp.sum(dout * start_o, axis=1, keepdims=True)
        dv_ref[:, r * DV : (r + 1) * DV] = b_c * dright
        db = (e2sum + dr_r) / b_c
        dg = e1sum + e2sum - tsum + do_y + (dr_r - b_c * dr_v)
        acc = acc_ref[...]
        acc = jnp.where(lane == h, dg, acc)
        acc_ref[...] = jnp.where(lane == 8 + h, db, acc)
    kf, qf = k.astype(F32), q.astype(F32)
    dk_ref[...] = rk_c * (dkh - kf * (rk_c * rk_c * jnp.sum(kf * dkh, axis=1, keepdims=True)))
    dq_ref[...] = rq_c * (
        dqh - qf * (rq_c * rq_c * DK * jnp.sum(qf * dqh, axis=1, keepdims=True))
    )

    @pl.when(kh == pl.num_programs(0) - 1)
    def _():
        acc_t = acc_ref[...].T
        tail = causal.astype(F32).astype(BF16)
        dd_ref[...] = exact_rows_dot(acc_t[0:8], tail)[0:heads]
        dw_ref[...] = acc_t[8 : 8 + heads]


def backward_prefix_kernel(
    k_ref, v_ref, rows_ref, cols_ref, nt_ref, u_ref, gs_ref, dk_in, dv_in, dw_in, dd_in,
    dk_ref, dv_ref, dw_ref, dd_ref,
):
    heads = u_ref.shape[0]
    key_heads = k_ref.shape[1] // DK
    rep = heads // key_heads
    n = SPAN
    ri, ci = iota2((n, n), 0), iota2((n, n), 1)
    causal, causal_t, off_diag = ri >= ci, ri <= ci, ri != ci
    cols = cols_ref[...]
    lane = iota2((n, 128), 1)
    acc = jnp.zeros((n, 128), F32)
    last_row = iota2((n, 1), 0) == n - 1
    for kh in range(key_heads):
        k = k_ref[:, kh * DK : (kh + 1) * DK]
        kf = k.astype(F32)
        kk = dot_nt(k, k)
        rk_c = col(cols, ROW_RK + kh)
        rk_r = rows_ref[ROW_RK + kh : ROW_RK + kh + 1, 0:n]
        dkh = jnp.zeros((n, DK), F32)
        for r in range(rep):
            h = kh * rep + r
            g_c, b_c = col(cols, ROW_G + h), col(cols, ROW_B + h)
            g_r = rows_ref[ROW_G + h : ROW_G + h + 1, 0:n]
            b_r = rows_ref[ROW_B + h : ROW_B + h + 1, 0:n]
            diff = g_c - g_r
            decay = jnp.exp(jnp.where(causal & off_diag, diff, -1e30))
            decay_t = jnp.exp(jnp.where(causal_t & off_diag, -diff, -1e30))
            rest = jnp.exp(g_c[n - 1 : n] - g_c)
            sh, sl = halves(gs_ref[h])
            u16 = u_ref[h]
            dupdate = (rest * rk_c) * (dot_nn(k, sh) + dot_nn(k, sl))
            dright = dupdate + dot_nn(nt_ref[h][:, 0:n], dupdate.astype(BF16))
            dr16 = dright.astype(BF16)
            p2 = dot_nt(dr16, u16) * (decay * (-b_c) * rk_r)
            p2t = dot_nt(u16, dr16) * (decay_t * (-b_r) * rk_r)
            e2sum = jnp.sum(p2 * kk, axis=1, keepdims=True) * rk_c
            tsum = jnp.sum(p2t * kk, axis=1, keepdims=True) * rk_c
            back = rest * (dot_nt(u16, sh) + dot_nt(u16, sl))
            dkh = dkh + back + dot_nn((p2 + p2t).astype(BF16), k)
            e3 = rk_c * jnp.sum(kf * back, axis=1, keepdims=True)
            vf = v_ref[:, h * DV : (h + 1) * DV].astype(F32)
            db = e2sum / b_c + jnp.sum(dright * vf, axis=1, keepdims=True)
            dg = e2sum - tsum - e3 + jnp.where(last_row, jnp.sum(e3), 0.0)
            dv_ref[:, h * DV : (h + 1) * DV] = dv_in[:, h * DV : (h + 1) * DV] + b_c * dright
            acc = jnp.where(lane == h, dg, acc)
            acc = jnp.where(lane == 8 + h, db, acc)
        dk_ref[:, kh * DK : (kh + 1) * DK] = dk_in[:, kh * DK : (kh + 1) * DK] + rk_c * (
            dkh - kf * (rk_c * rk_c * jnp.sum(kf * dkh, axis=1, keepdims=True))
        )
    acc_t = jnp.concatenate([acc, jnp.zeros((128 - n, 128), F32)], axis=0).T
    si, sj = iota2((128, 128), 0), iota2((128, 128), 1)
    tail = ((si >= sj) & (si < n)).astype(F32).astype(BF16)
    dd_ref[...] = dd_in[...] + exact_rows_dot(acc_t[0:8], tail)[0:heads]
    dw_ref[...] = dw_in[...] + acc_t[8 : 8 + heads]


HEAD_REP = [2]


def swap(x, bit, axis, size):
    return lax.ppermute(x, axis, [(i, i ^ bit) for i in range(size)])


def shift(x, by, axis, size):
    return lax.ppermute(x, axis, [(i, (i + by) % size) for i in range(size)])


def gather_states(x, size):
    if size > 8:
        return lax.all_gather(x, "seq", axis=0)
    me = lax.axis_index("seq")
    out = jnp.zeros((size,) + x.shape, x.dtype)
    out = lax.dynamic_update_index_in_dim(out, x, me, 0)
    for bit in range(1, size):
        out = lax.dynamic_update_index_in_dim(out, swap(x, bit, "seq", size), me ^ bit, 0)
    return out


def gather_heads(x, size):
    me = lax.axis_index("head")
    out = jnp.zeros((size,) + x.shape, x.dtype)
    out = lax.dynamic_update_index_in_dim(out, x, me, 0)
    for by in range(1, size):
        out = lax.dynamic_update_index_in_dim(
            out, shift(x, by, "head", size), (me - by) % size, 0
        )
    return out


def scatter_heads(parts, size):
    me = lax.axis_index("head")
    total = lax.dynamic_index_in_dim(parts, me, 0, False).astype(F32)
    for by in range(1, size):
        part = lax.dynamic_index_in_dim(parts, (me + by) % size, 0, False)
        total = total + shift(part, by, "head", size).astype(F32)
    return total


def take_half(v, axis, which):
    return lax.dynamic_index_in_dim(v, which, axis, False)


def fold(v, axis, bit, dist, size):
    mine = take_half(v, axis, bit).astype(F32)
    return mine + swap(take_half(v, axis, 1 - bit), dist, "seq", size).astype(F32)


def scatter_seq(x, size):
    if size != 8:
        return lax.psum_scatter(x, "seq", scatter_dimension=0, tiled=False).astype(F32)
    me = lax.axis_index("seq")
    c, xb, yb = me & 1, (me >> 1) & 1, (me >> 2) & 1
    v = x.reshape((2, 2, 2) + x.shape[1:])
    a = fold(v, 2, c, 1, size).astype(x.dtype)
    half = a.shape[2] // 2
    first = fold(a[:, :, :half], 1, xb, 2, size).astype(x.dtype)
    second = fold(a[:, :, half:], 0, yb, 4, size).astype(x.dtype)
    first = fold(first, 0, yb, 4, size)
    second = fold(second, 0, xb, 2, size)
    return jnp.concatenate([first, second], axis=0)


def per_device(
    n_seq, n_head, query, key, value, gate, write, decay, weight, cotangent, br, po
):
    rows = query.shape[0]
    heads = write.shape[0]
    key_heads = query.shape[1] // DK
    rep = heads // key_heads
    HEAD_REP[0] = rep
    sds = jax.ShapeDtypeStruct
    width = weight.shape[0]
    cut = width // n_head

    cot = gather_heads(cotangent, n_head)
    weight4 = weight.reshape(n_head, cut, weight.shape[1])

    def whole(*shape):
        return pl.BlockSpec(shape, lambda *_: (0,) * len(shape))

    def call(body, prefetch, grid, ins, outs, shapes, args, scratch=(), aliases=None, flops=10**8):
        return pl.pallas_call(
            body,
            grid_spec=pltpu.PrefetchScalarGridSpec(
                num_scalar_prefetch=prefetch, grid=grid, in_specs=ins, out_specs=outs,
                scratch_shapes=list(scratch),
            ),
            out_shape=shapes,
            input_output_aliases=aliases or {},
            cost_estimate=pl.CostEstimate(flops=flops, transcendentals=0, bytes_accessed=10**6),
            name=body.__name__,
        )(*args)

    rows_tab, cols_tab, state = call(
        prefix_kernel, 1, (1,),
        [whole(rows, key_heads * DK), whole(rows, key_heads * DK), whole(SPAN, heads * DV),
         whole(heads, rows), whole(heads, rows)],
        [whole(ROW_END, rows), whole(rows, 128), whole(heads, DK, DV)],
        [sds((ROW_END, rows), F32), sds((rows, 128), F32), sds((heads, DK, DV), BF16)],
        (br, query, key, value, write, decay),
    )
    states = gather_states(state, n_seq)

    by_key = pl.BlockSpec((rows, DK), lambda h, *_: (0, h))
    square = pl.BlockSpec((rep, rows, rows), lambda h, *_: (h, 0, 0))
    tables = [whole(ROW_END, rows), whole(rows, 128)]
    nmat, nmat_t, mmat, mmat_t = call(
        system_kernel, 1, (key_heads,), [by_key, by_key] + tables, [square] * 4,
        [sds((heads, rows, rows), BF16)] * 4, (br, query, key, rows_tab, cols_tab),
    )

    key_of = pl.BlockSpec((rows, DK), lambda h, *_: (0, h // rep))
    by_head = pl.BlockSpec((rows, DV), lambda h, *_: (0, h))
    square1 = pl.BlockSpec((1, rows, rows), lambda h, *_: (h, 0, 0))
    rows1 = pl.BlockSpec((1, rows, DV), lambda h, *_: (h, 0, 0))
    states1 = pl.BlockSpec((n_seq, 1, DK, DV), lambda h, *_: (0, h, 0, 0))
    per_head32 = sds((heads, rows, DV), F32)
    flat32 = sds((rows, heads * DV), F32)
    normed, outs, update, right, start_o = call(
        forward_kernel, 2, (heads,),
        [key_of, key_of, by_head, by_head, whole(rows, 128), square1, square1, states1],
        [by_head, by_head, rows1, rows1, rows1],
        [sds((rows, heads * DV), BF16), flat32, sds((heads, rows, DV), BF16), per_head32, per_head32],
        (br, po, query, key, value, gate, cols_tab, nmat, mmat, states),
    )

    grad_normed = jnp.einsum("jrd,jdv->rv", cot, weight4, preferred_element_type=F32)
    grad_weight = scatter_seq(
        jnp.einsum("jrd,rv->jdv", cot, normed, preferred_element_type=F32)
        .astype(BF16)
        .reshape(n_seq, width // n_seq, -1),
        n_seq,
    )
    layer_out = scatter_heads(
        jnp.einsum("rv,jdv->jrd", normed, weight4, preferred_element_type=F32).astype(BF16), n_head
    ).astype(BF16)

    grad_gate, dout, dright, gs = call(
        backward_state_kernel, 2, (heads,),
        [key_of, key_of, by_head, by_head, by_head, whole(rows, 128), square1, square1],
        [by_head, rows1, rows1, states1],
        [flat32, per_head32, per_head32, sds((n_seq, heads, DK, DV), BF16)],
        (br, po, query, key, gate, grad_normed, outs, cols_tab, nmat_t, mmat_t),
    )
    own = scatter_seq(gs.reshape(n_seq, heads * DK, DV), n_seq).reshape(heads, DK, DV)

    wide_v = pl.BlockSpec((rows, rep * DV), lambda h, *_: (0, h))
    rows_rep = pl.BlockSpec((rep, rows, DV), lambda h, *_: (h, 0, 0))
    states_rep = pl.BlockSpec((n_seq, rep, DK, DV), lambda h, *_: (0, h, 0, 0))
    keys32 = sds((rows, key_heads * DK), F32)
    small32 = sds((heads, rows), F32)
    dq, dk, dv, dw, dd = call(
        backward_rest_kernel, 2, (key_heads,),
        [by_key, by_key, wide_v] + tables + [states_rep] + [rows_rep] * 5,
        [by_key, by_key, wide_v, whole(heads, rows), whole(heads, rows)],
        [keys32, keys32, flat32, small32, small32],
        (br, po, query, key, value, rows_tab, cols_tab, states, dout, dright, update, right, start_o),
        scratch=[pltpu.VMEM((rows, 128), F32)],
    )
    dk, dv, dw, dd = call(
        backward_prefix_kernel, 0, (1,),
        [whole(SPAN, key_heads * DK), whole(SPAN, heads * DV), whole(ROW_END, 128),
         whole(SPAN, 128), whole(heads, SPAN, 128), whole(heads, SPAN, DV), whole(heads, DK, DV),
         whole(SPAN, key_heads * DK), whole(SPAN, heads * DV), whole(heads, 128), whole(heads, 128)],
        [whole(SPAN, key_heads * DK), whole(SPAN, heads * DV), whole(heads, 128), whole(heads, 128)],
        [keys32, flat32, small32, small32],
        (key, value, rows_tab, cols_tab, nmat_t, update, own, dk, dv, dw, dd),
        aliases={7: 0, 8: 1, 9: 2, 10: 3},
    )
    return layer_out, dq, dk, dv, grad_gate, dw, dd, grad_weight


def solution(mesh):
    n_seq, n_head = mesh.shape["seq"], mesh.shape["head"]
    both, turned = P("seq", "head"), P("head", "seq")
    return jax.shard_map(
        partial(per_device, n_seq, n_head),
        mesh=mesh,
        in_specs=(both, both, both, both, turned, turned, P(None, "head"), both, P(), P()),
        out_specs=(both, both, both, both, both, turned, turned, both),
        check_vma=False,
    )
```
